32 devices in a mesh: groups: 2 (over y), seq: 4 (over z), head: 2 (over x), rep: 2 (over core).
Axes of the slice: x: 2, y: 2, z: 4, core: 2. Of those that a mesh axis runs over, the one named last changes fastest.
Arguments:
- tokens: bfloat16 [8, 4096], P('groups', ('seq', 'rep')), parts along dimension 0, may hold values from -6 to 6
- attn_gain: float32 [4096], P(('seq', 'rep')), may hold values from 0.25 to 1.75
- ffn_gain: float32 [4096], P(('seq', 'rep')), may hold values from 0.25 to 1.75
- w_query: bfloat16 [4096, 4096], P(('seq', 'rep'), 'head'), may hold values from -0.0625 to 0.0625
- w_key: bfloat16 [4096, 1024], P(('seq', 'rep'), 'head'), may hold values from -0.09375 to 0.09375
- w_value: bfloat16 [4096, 1024], P(('seq', 'rep'), 'head'), may hold values from -0.25 to 0.25
- w_out: bfloat16 [4096, 4096], P('head', ('seq', 'rep')), may hold values from -0.09375 to 0.09375
- w_gate: bfloat16 [4096, 7168], P(('seq', 'rep'), 'head'), may hold values from -0.09375 to 0.09375
- w_up: bfloat16 [4096, 7168], P(('seq', 'rep'), 'head'), may hold values from -0.09375 to 0.09375
- w_down: bfloat16 [7168, 4096], P('head', ('seq', 'rep')), may hold values from -0.0625 to 0.0625
- kv_pool: bfloat16 [2, 8, 4, 128, 1024], P(None, ('groups', 'seq'), 'head', 'rep'), parts along dimension 1, may hold values from -15 to 15
- lengths: int32 [8], P('groups'), parts along dimension 0, may hold values from 1 to 512, 1024 in all
- pool_row: int32 [8], P('groups'), parts along dimension 0, may hold values from 0 to 3, each once
- block_table: int32 [8, 4], P('groups'), parts along dimension 0, may hold values from 0 to 3, each once within a row
Outputs:
- layer_out: bfloat16 [8, 4096], P('groups', ('seq', 'rep')), parts along dimension 0
- kv_decode: bfloat16 [2, 8, 512, 1024], P(None, 'groups', ('seq', 'rep'), 'head'), parts along dimension 1
The draws below stay inside these ranges and needn't reach their ends.
There are 2 independent parts, one for each index of `groups`. The reference program is written for one: setup_inputs(seed, part) draws one part's arguments, and reference() takes and returns one part's arrays. A program takes and returns all parts, laid end to end along the dimension named above; an argument that names none is the same for every part. Nothing has to cross between parts.
Inputs may be any that keep to these rules, and one draw needn't show every extreme that they name: One sequence reaches 512; the lengths sum to 1024. `pool_row`: a permutation of the pool rows. `block_table`: every row is a permutation of the 4 slots.
All inputs are finite; a program needn't handle non-finite values.
Results may differ from the reference program's by a relative error of at most 0.008.
Values may be sent and summed in bfloat16 or wider, within the bound.
A program may use at most 64 MiB of HBM per device.

```python
import math
import jax
import jax.numpy as jnp
import numpy as np
from jax import lax

D = 4096
H = 32
KVH = 8
HD = 128
FFW = 7168
BLK = 128
SEQS = 4
MAXBLK = 4
MAXLEN = 512


def draw_tokens(key, part):
    values = jax.random.normal(key, (SEQS, D), jnp.float32)
    return jnp.clip(values, -6.0, 6.0).astype(jnp.bfloat16)


def draw_w_query(key, part):
    spread = D ** (-0.5)
    values = jax.random.normal(key, (D, H * HD), jnp.float32) * spread
    return jnp.clip(values, -4.0 * spread, 4.0 * spread).astype(jnp.bfloat16)


def draw_kv_pool(key, part):
    width = KVH * HD
    values = jax.random.normal(key, (2, SEQS, MAXBLK, BLK, width), jnp.float32) * 2.5
    return jnp.clip(values, -15.0, 15.0).astype(jnp.bfloat16)


def level_of(rng, dims, shards, low, high):
    def one(position, parts):
        heights = jax.random.uniform(jax.random.fold_in(jax.random.fold_in(rng, 6), position), (parts,), jnp.float32, low / len(shards), high / len(shards))
        return jnp.repeat(jnp.exp(heights), dims[position] // parts).reshape((-1,) + (1,) * (len(dims) - position - 1))

    factor_of = one(*shards[0])
    for cut in shards[1:]:
        factor_of = factor_of * one(*cut)
    return factor_of


def split_up(count, total, reach, slope):
    portions = [(1 << 20) // math.isqrt(rank ** slope) + 1 for rank in range(2, count + 1)]
    surplus, given = total - reach - (count - 1), [1] * (count - 1)
    while surplus > 0:
        movable = [i for i in range(count - 1) if given[i] < reach]
        mass, left = sum([portions[i] for i in movable]), surplus
        for i in movable:
            extra = min(reach - given[i], max(1, left * portions[i] // mass), surplus)
            given[i] = given[i] + extra
            surplus = surplus - extra
    return np.array([reach] + given)


def uneven(rng, count, total, limit, slope):
    if count == 2:
        one = jax.random.randint(rng, (), max(1, total - limit), min(limit, total - 1) + 1)
        return jnp.stack([one, total - one])
    tallies = jnp.asarray(split_up(count, total, limit, slope), jnp.int32)
    couples = (count - 1) // 2
    source_of, sink = tallies[1:1 + 2 * couples:2], tallies[2:2 + 2 * couples:2]
    margin = jnp.minimum(source_of - 1, limit - sink)
    passed = jax.random.randint(jax.random.fold_in(rng, 1), (couples,), 0, 1 << 20) % (margin + 1)
    tallies = tallies.at[1:1 + 2 * couples:2].set(source_of - passed).at[2:2 + 2 * couples:2].set(sink + passed)
    return tallies[jax.random.permutation(jax.random.fold_in(rng, 2), count)]


def bell_draw(own_key, dims, scale, limit, split=(), kind=jnp.bfloat16):
    entries = jax.random.normal(own_key, dims, jnp.float32) * scale
    if len(split) > 0:
        entries = level_of(own_key, dims, split, -0.22, 0.18) * entries
    return jnp.clip(entries, min=-limit, max=limit).astype(kind)


def setup_inputs(seed: int = 0, part: int = 0) -> dict:
    splits = jax.random.split(jax.random.key(seed), 15)
    own_keys = jax.random.split(jax.random.fold_in(splits[14], part), 15)
    return {
        "tokens": draw_tokens(jax.random.fold_in(jax.random.fold_in(splits[14], part), 71), part),
        "attn_gain": jnp.clip(1.0 + 0.15 * jax.random.normal(splits[1], (D,), jnp.float32), 0.25, 1.75),
        "ffn_gain": jnp.clip(1.0 + 0.15 * jax.random.normal(splits[2], (D,), jnp.float32), 0.25, 1.75),
        "w_query": draw_w_query(jax.random.fold_in(splits[14], 71), part),
        "w_key": bell_draw(splits[4], (D, KVH * HD), D ** -0.5, 0.09375, ((0, 8), (1, 2))),
        "w_value": bell_draw(splits[5], (D, KVH * HD), (D // 8) ** -0.5, 0.25, ((0, 8), (1, 2))),
        "w_out": bell_draw(splits[6], (H * HD, D), (H * HD) ** -0.5, 0.09375, ((0, 2), (1, 8))),
        "w_gate": bell_draw(splits[7], (D, FFW), D ** -0.5, 0.09375, ((0, 8), (1, 2))),
        "w_up": bell_draw(splits[8], (D, FFW), D ** -0.5, 0.09375, ((0, 8), (1, 2))),
        "w_down": bell_draw(splits[9], (FFW, D), FFW ** -0.5, 0.0625, ((0, 2), (1, 8))),
        "kv_pool": draw_kv_pool(jax.random.fold_in(jax.random.fold_in(splits[14], part), 71), part),
        "lengths": uneven(own_keys[11], SEQS, SEQS * MAXLEN // 2, MAXLEN, 2).astype(jnp.int32),
        "pool_row": jax.random.permutation(own_keys[12], SEQS).astype(jnp.int32),
        "block_table": jax.vmap(lambda own: jax.random.permutation(own, MAXBLK))(jax.random.split(own_keys[13], SEQS)).reshape((SEQS, MAXBLK)).astype(jnp.int32),
    }


EPSILON = 1e-05
ROPE_LOG = math.log(500000.0)
FLOOR_SCORE = -1e+30

def rms_scale(residual, gain):
    squares = lax.optimization_barrier(jnp.sum(residual * residual, axis=-1))
    return residual * lax.rsqrt(squares / D + EPSILON)[:, None] * gain

def rotate(values, positions):
    half_dim = values.shape[-1] // 2
    freq_table = jnp.exp(jnp.arange(half_dim, dtype=jnp.float32) * (-2.0 * ROPE_LOG / values.shape[-1]))
    angles = positions[:, None, None] * freq_table
    cosine = jnp.cos(angles)
    sine_part = jnp.sin(angles)
    first_half = values[..., :half_dim]
    second_half = values[..., half_dim:]
    return jnp.concatenate([first_half * cosine - second_half * sine_part, second_half * cosine + first_half * sine_part], axis=-1)

def reference(tokens, attn_gain, ffn_gain, w_query, w_key, w_value, w_out, w_gate, w_up, w_down, kv_pool, lengths, pool_row, block_table):
    residual = tokens.astype(jnp.float32)
    normed = rms_scale(residual, attn_gain).astype(jnp.bfloat16)
    queries = jnp.dot(normed, w_query, preferred_element_type=jnp.float32).reshape(SEQS, H, HD)
    keys_new = jnp.dot(normed, w_key, preferred_element_type=jnp.float32).reshape(SEQS, KVH, HD)
    values_new = jnp.dot(normed, w_value, preferred_element_type=jnp.float32).reshape(SEQS, KVH, HD)
    positions = lengths.astype(jnp.float32)
    rot_queries = rotate(queries, positions).astype(jnp.bfloat16)
    rot_keys = rotate(keys_new, positions).astype(jnp.bfloat16)
    new_values = values_new.astype(jnp.bfloat16)
    pool_rows = jnp.take(kv_pool, pool_row.astype(jnp.int32), axis=1)
    ordered = jax.vmap(lambda row_blocks, table_row: jnp.take(row_blocks, table_row, axis=1), in_axes=(1, 0), out_axes=1)(pool_rows, block_table.astype(jnp.int32))
    cache = ordered.reshape(2, SEQS, MAXLEN, KVH * HD)
    is_live = jnp.arange(MAXLEN, dtype=jnp.int32)[None, :] < lengths[:, None]
    kv_decode = jnp.where(is_live[None, :, :, None], cache, jnp.zeros((), jnp.bfloat16))
    factor = 1.0 / math.sqrt(HD)
    per_group = H // KVH

    def attend(record):
        query_row, key_own, value_own, key_rows, value_rows, usable = record
        query_f = query_row.astype(jnp.float32).reshape(KVH, per_group, HD)
        key_f = key_rows.astype(jnp.float32).reshape(MAXLEN, KVH, HD)
        value_f = value_rows.astype(jnp.float32).reshape(MAXLEN, KVH, HD)
        scores = jnp.einsum('ngd,tnd->ngt', query_f, key_f) * factor
        scores = jnp.where(usable[None, None, :], scores, FLOOR_SCORE)
        own_score = lax.optimization_barrier(jnp.sum(query_f * key_own.astype(jnp.float32)[:, None, :], axis=-1)) * factor
        largest = jnp.maximum(lax.optimization_barrier(jnp.max(scores, axis=-1)), own_score)
        weights = jnp.where(usable[None, None, :], jnp.exp(scores - largest[..., None]), 0.0)
        own_weight = jnp.exp(own_score - largest)
        denominator = lax.optimization_barrier(jnp.sum(weights, axis=-1)) + own_weight
        rounded = lax.optimization_barrier(weights.astype(jnp.bfloat16)).astype(jnp.float32)
        mixed = jnp.einsum('ngt,tnd->ngd', rounded, value_f) + own_weight[..., None] * value_own.astype(jnp.float32)[:, None, :]
        return (mixed / denominator[..., None]).reshape(H * HD)
    attn = lax.map(attend, (rot_queries, rot_keys, new_values, kv_decode[0], kv_decode[1], is_live)).astype(jnp.bfloat16)
    middle = residual + jnp.dot(attn, w_out, preferred_element_type=jnp.float32)
    normed_mid = rms_scale(middle, ffn_gain).astype(jnp.bfloat16)
    gate_sum = jnp.dot(normed_mid, w_gate, preferred_element_type=jnp.float32)
    up_sum = jnp.dot(normed_mid, w_up, preferred_element_type=jnp.float32)
    hidden = (jax.nn.silu(gate_sum) * up_sum).astype(jnp.bfloat16)
    layer_out = (middle + jnp.dot(hidden, w_down, preferred_element_type=jnp.float32)).astype(jnp.bfloat16)
    return (layer_out, kv_decode)
```

```python
import functools
import math

import jax
import jax.numpy as jnp
from jax import lax
from jax.experimental import pallas as pl
from jax.experimental.pallas import tpu as pltpu
from jax.sharding import PartitionSpec as P

HD = 128
EPSILON = 1e-05
ROPE_LOG = math.log(500000.0)
FLOOR_SCORE = -1e30
MESH = pl.DeviceIdType.MESH
F32 = jnp.float32
BF16 = jnp.bfloat16


def trig_rows(lengths):
    half_dim = HD // 2
    freq_table = jnp.exp(jnp.arange(half_dim, dtype=F32) * (-2.0 * ROPE_LOG / HD))
    angles = lengths.astype(F32)[:, None] * freq_table
    cosine = jnp.cos(angles)
    sine_part = jnp.sin(angles)
    return jnp.concatenate([cosine, cosine, -sine_part, sine_part], axis=-1)


def layer_kernel(
    dims,
    lengths_ref,
    row_ref,
    table_ref,
    trig_ref,
    tokens_ref,
    gain_ref,
    ffn_gain_ref,
    wq_hbm,
    wk_hbm,
    wv_hbm,
    wo_hbm,
    wg_hbm,
    wu_hbm,
    wd_hbm,
    pool_hbm,
    out_ref,
    kv_ref,
    wq,
    wk,
    wv,
    wo,
    wg,
    wu,
    wd,
    kvx,
    kvs,
    arr,
    tok,
    xp,
    qkv_part,
    qkv_recv,
    heads_buf,
    soft_part,
    soft_recv,
    attn_part,
    attn_recv,
    attn_rows,
    proj_part,
    proj_recv,
    mid_part,
    mid_recv,
    hid_part,
    hid_recv,
    hid_rows,
    down_part,
    down_recv,
    final,
    local_sem,
    kvx_send,
    kvx_recv,
    kvz_send,
    kvz_recv,
    qkv_send,
    qkv_rsem,
    soft_send,
    soft_rsem,
    attn_send,
    attn_rsem,
    proj_send,
    proj_rsem,
    mid_send,
    mid_rsem,
    hid_send,
    hid_rsem,
    down_send,
    down_rsem,
):
    n_seq, n_head, n_rep, width, block = dims
    seq_count = tokens_ref.shape[0]
    group = lax.axis_index("groups")
    s_me = lax.axis_index("seq")
    h_me = lax.axis_index("head")
    r_me = lax.axis_index("rep")
    n_ring = n_seq * n_rep
    me = s_me * n_rep + r_me

    def at_ring(peer):
        return (group, peer // n_rep, h_me, peer % n_rep)

    def at_head(peer):
        return (group, s_me, peer, r_me)

    def at_seq(peer):
        return (group, peer, h_me, r_me)

    def at_rep(peer):
        return (group, s_me, h_me, peer)

    def send_all(source_of, dst, count, mine, place, send, recv):
        copies = []
        for k in range(1, count):
            peer = lax.rem(mine + k, count)
            copy = pltpu.make_async_remote_copy(
                src_ref=source_of(peer),
                dst_ref=dst.at[mine],
                send_sem=send.at[k],
                recv_sem=recv.at[k],
                device_id=place(peer),
                device_id_type=MESH,
            )
            copy.start()
            copies.append(copy)
        return copies

    def arrive(copies):
        for copy in copies:
            copy.wait()

    half_feat = pool_hbm.shape[4] // n_head
    weights = []
    for j, (src, dst) in enumerate(
        ((wq_hbm, wq), (wk_hbm, wk), (wv_hbm, wv), (wo_hbm, wo), (wg_hbm, wg), (wu_hbm, wu), (wd_hbm, wd))
    ):
        copy = pltpu.make_async_copy(src, dst, local_sem.at[j])
        copy.start()
        weights.append(copy)

    def features_for(peer):
        return pool_hbm.at[:, 0, :, :, pl.ds(pl.multiple_of(peer * half_feat, HD), half_feat)]

    own_kv = pltpu.make_async_copy(features_for(h_me), kvx.at[h_me], local_sem.at[7])
    own_kv.start()

    barrier = pltpu.get_barrier_semaphore()
    for k in range(1, n_ring):
        pl.semaphore_signal(
            barrier, inc=1, device_id=at_ring(lax.rem(me + k, n_ring)), device_id_type=MESH
        )
    for k in range(1, n_head):
        pl.semaphore_signal(
            barrier, inc=1, device_id=at_head(lax.rem(h_me + k, n_head)), device_id_type=MESH
        )
    pl.semaphore_wait(barrier, n_ring + n_head - 2)

    kvx_copies = send_all(features_for, kvx, n_head, h_me, at_head, kvx_send, kvx_recv)

    tok[...] = tokens_ref[...].astype(F32)
    owner_here = jnp.int32(0)
    for p in range(seq_count):
        owner = jnp.int32(0)
        for i in range(seq_count):
            owner = jnp.where(row_ref[i] == p, i, owner)
        owner_here = jnp.where(s_me == p, owner, owner_here)
        xp[p : p + 1, :] = tok[pl.ds(owner, 1), :]
    length_here = lengths_ref[owner_here]

    residual = xp[...]
    squares = jnp.sum(residual * residual, axis=1, keepdims=True)
    scaled = (residual * gain_ref[...]).astype(BF16)
    q_cols, kv_cols = wq.shape[1], wk.shape[1]
    for copy in weights[:3]:
        copy.wait()
    q_part = jnp.dot(scaled, wq[...], preferred_element_type=F32)
    k_part = jnp.dot(scaled, wk[...], preferred_element_type=F32)
    v_part = jnp.dot(scaled, wv[...], preferred_element_type=F32)
    total = q_cols + 2 * kv_cols
    for s in range(seq_count):
        qkv_part[s, :, 0:q_cols] = q_part[s : s + 1]
        qkv_part[s, :, q_cols : q_cols + kv_cols] = k_part[s : s + 1]
        qkv_part[s, :, q_cols + kv_cols : total] = v_part[s : s + 1]
        qkv_part[s, :, total : total + HD] = jnp.broadcast_to(squares[s : s + 1], (1, HD))
    qkv_copies = send_all(
        lambda peer: qkv_part.at[peer // n_rep], qkv_recv, n_ring, me, at_ring, qkv_send, qkv_rsem
    )
    qkv_recv[me] = qkv_part[s_me]

    own_kv.wait()
    arrive(kvx_copies)
    slots_local = kvx.shape[2]
    half_rows = kvx.shape[3]
    blocks = table_ref.shape[1]
    for b in range(blocks):
        slot = table_ref[owner_here, b]
        holder = slot // slots_local
        local = lax.rem(slot, slots_local)
        first = b * block + r_me * half_rows
        live = lax.broadcasted_iota(jnp.int32, (half_rows, half_feat), 0) + first < length_here
        for c in range(2):
            rows = kvx[holder, c, local].astype(F32)
            kvs[b, c] = jnp.where(live, rows, 0.0).astype(BF16)

    arrive(qkv_copies)
    summed = jnp.sum(qkv_recv[...], axis=0)
    scale = lax.rsqrt(summed[:, total : total + HD] / width + EPSILON)
    heads = q_cols // HD
    kv_heads = kv_cols // HD
    for h in range(heads + 2 * kv_heads):
        heads_buf[h : h + 1, :] = summed[:, h * HD : (h + 1) * HD] * scale
    trig = trig_ref[pl.ds(owner_here, 1), :]
    queries = heads_buf[0:heads]
    keys_new = heads_buf[heads : heads + kv_heads]
    values_new = heads_buf[heads + kv_heads : heads + 2 * kv_heads].astype(BF16).astype(F32)

    def rotated(values):
        return (values * trig[:, :HD] + pltpu.roll(values, HD // 2, 1) * trig[:, HD:]).astype(BF16)

    rot_queries = rotated(queries)
    rot_keys = rotated(keys_new).astype(F32)
    factor = 1.0 / math.sqrt(HD)
    per_group = heads // kv_heads
    tokens_here = blocks * half_rows
    spot = lax.broadcasted_iota(jnp.int32, (per_group, tokens_here), 1)
    position = (spot // half_rows) * block + lax.rem(spot, half_rows) + r_me * half_rows
    usable = position < length_here
    for g in range(kv_heads):
        cols = slice(g * HD, (g + 1) * HD)
        mine = slice(g * per_group, (g + 1) * per_group)
        keys = kvs[:, 0, :, cols].reshape(tokens_here, HD)
        values = kvs[:, 1, :, cols].reshape(tokens_here, HD)
        scores = (
            lax.dot_general(
                rot_queries[mine], keys, (((1,), (1,)), ((), ())), preferred_element_type=F32
            )
            * factor
        )
        scores = jnp.where(usable, scores, FLOOR_SCORE)
        highest = jnp.max(scores, axis=1, keepdims=True)
        shares = jnp.where(usable, jnp.exp(scores - highest), 0.0)
        mass = jnp.sum(shares, axis=1, keepdims=True)
        soft_part[0, mine, :] = jnp.dot(shares.astype(BF16), values, preferred_element_type=F32)
        soft_part[1, mine, :] = jnp.broadcast_to(highest, (per_group, HD))
        soft_part[2, mine, :] = jnp.broadcast_to(mass, (per_group, HD))
    soft_copies = send_all(
        lambda peer: soft_part, soft_recv, n_rep, r_me, at_rep, soft_send, soft_rsem
    )
    soft_recv[r_me] = soft_part[...]
    own_key = jnp.concatenate(
        [jnp.broadcast_to(rot_keys[g : g + 1], (per_group, HD)) for g in range(kv_heads)], axis=0
    )
    own_value = jnp.concatenate(
        [jnp.broadcast_to(values_new[g : g + 1], (per_group, HD)) for g in range(kv_heads)], axis=0
    )
    own_score = jnp.sum(rot_queries.astype(F32) * own_key, axis=1, keepdims=True) * factor
    arrive(soft_copies)
    largest = jnp.broadcast_to(own_score, (heads, HD))
    for r in range(n_rep):
        largest = jnp.maximum(largest, soft_recv[r, 1])
    own_share = jnp.exp(own_score - largest)
    denominator = own_share
    mixed = own_share * own_value
    for r in range(n_rep):
        weight = jnp.exp(soft_recv[r, 1] - largest)
        denominator = denominator + soft_recv[r, 2] * weight
        mixed = mixed + soft_recv[r, 0] * weight
    attn_part[...] = (mixed / denominator).astype(BF16).astype(F32)
    attn_copies = send_all(
        lambda peer: attn_part, attn_recv, n_seq, s_me, at_seq, attn_send, attn_rsem
    )
    attn_recv[s_me] = attn_part[...]
    kvz_copies = send_all(lambda peer: kvs.at[peer], arr, n_seq, s_me, at_seq, kvz_send, kvz_recv)
    arr[s_me] = kvs[s_me]
    weights[3].wait()
    arrive(attn_copies)
    for s in range(seq_count):
        for h in range(heads):
            attn_rows[s : s + 1, h * HD : (h + 1) * HD] = attn_recv[s, h : h + 1, :]
    proj_part[...] = jnp.dot(attn_rows[...].astype(BF16), wo[...], preferred_element_type=F32)
    proj_copies = send_all(
        lambda peer: proj_part, proj_recv, n_head, h_me, at_head, proj_send, proj_rsem
    )
    proj_recv[h_me] = proj_part[...]
    for copy in weights[4:6]:
        copy.wait()
    arrive(proj_copies)
    middle = xp[...] + jnp.sum(proj_recv[...], axis=0)
    mid_squares = jnp.sum(middle * middle, axis=1, keepdims=True)
    mid_scaled = (middle * ffn_gain_ref[...]).astype(BF16)
    piece = wg.shape[1] // n_rep
    for j, weight in enumerate((wg, wu)):
        partial = jnp.dot(mid_scaled, weight[...], preferred_element_type=F32)
        for s in range(seq_count):
            for r in range(n_rep):
                mid_part[s * n_rep + r, :, j * piece : (j + 1) * piece] = partial[
                    s : s + 1, r * piece : (r + 1) * piece
                ]
    for s in range(seq_count):
        for r in range(n_rep):
            mid_part[s * n_rep + r, :, 2 * piece : 2 * piece + HD] = jnp.broadcast_to(
                mid_squares[s : s + 1], (1, HD)
            )
    mid_copies = send_all(
        lambda peer: mid_part.at[peer], mid_recv, n_ring, me, at_ring, mid_send, mid_rsem
    )
    mid_recv[me] = mid_part[me]
    arrive(mid_copies)
    sums = jnp.sum(mid_recv[...], axis=0)
    mid_scale = lax.rsqrt(sums[:, 2 * piece : 2 * piece + 1] / width + EPSILON)
    gate = sums[:, :piece] * mid_scale
    up = sums[:, piece : 2 * piece] * mid_scale
    hid_part[...] = (gate / (1.0 + jnp.exp(-gate)) * up).astype(BF16).astype(F32)
    hid_copies = send_all(
        lambda peer: hid_part, hid_recv, n_ring, me, at_ring, hid_send, hid_rsem
    )
    hid_recv[me] = hid_part[...]
    weights[6].wait()
    arrive(hid_copies)
    for s in range(seq_count):
        for r in range(n_rep):
            hid_rows[s : s + 1, r * piece : (r + 1) * piece] = hid_recv[s * n_rep + r]
    down_part[...] = jnp.dot(hid_rows[...].astype(BF16), wd[...], preferred_element_type=F32)
    down_copies = send_all(
        lambda peer: down_part, down_recv, n_head, h_me, at_head, down_send, down_rsem
    )
    down_recv[h_me] = down_part[...]
    arrive(kvz_copies)
    for i in range(seq_count):
        source = row_ref[i]
        for c in range(2):
            kv_ref[c, i] = arr[source, c]
    arrive(down_copies)
    final[...] = middle + jnp.sum(down_recv[...], axis=0)
    for i in range(seq_count):
        tok[i : i + 1, :] = final[pl.ds(row_ref[i], 1), :]
    out_ref[...] = tok[...].astype(BF16)


def shards(
    n_groups,
    n_seq,
    n_head,
    n_rep,
    tokens,
    attn_gain,
    ffn_gain,
    w_query,
    w_key,
    w_value,
    w_out,
    w_gate,
    w_up,
    w_down,
    kv_pool,
    lengths,
    pool_row,
    block_table,
):
    seq_count, cols = tokens.shape
    n_ring = n_seq * n_rep
    width = cols * n_ring
    _, _, slots_local, half_rows, feat = kv_pool.shape
    half_feat = feat // n_head
    blocks = block_table.shape[1]
    q_cols, kv_cols = w_query.shape[1], w_key.shape[1]
    heads, kv_heads = q_cols // HD, kv_cols // HD
    qkv = q_cols + 2 * kv_cols + HD
    piece = w_gate.shape[1] // n_rep
    vmem = pltpu.VMEM
    dma = pltpu.SemaphoreType.DMA
    hbm = pl.BlockSpec(memory_space=pltpu.HBM)
    in_v = pl.BlockSpec(memory_space=pltpu.VMEM)
    in_s = pl.BlockSpec(memory_space=pltpu.SMEM)
    weights = (w_query, w_key, w_value, w_out, w_gate, w_up, w_down)
    out, kv = pl.pallas_call(
        functools.partial(layer_kernel, (n_seq, n_head, n_rep, width, half_rows * n_rep)),
        out_shape=(
            jax.ShapeDtypeStruct((seq_count, cols), BF16),
            jax.ShapeDtypeStruct((2, seq_count, half_rows, half_feat), BF16),
        ),
        in_specs=[in_s] * 3 + [in_v] * 4 + [hbm] * 8,
        out_specs=(in_v, in_v),
        scratch_shapes=[vmem(w.shape, BF16) for w in weights]
        + [
            vmem((n_head, 2, slots_local, half_rows, half_feat), BF16),
            vmem((blocks, 2, half_rows, half_feat), BF16),
            vmem((n_seq, 2, half_rows, half_feat), BF16),
            vmem((seq_count, cols), F32),
            vmem((seq_count, cols), F32),
            vmem((seq_count, 1, qkv), F32),
            vmem((n_ring, 1, qkv), F32),
            vmem((heads + 2 * kv_heads, HD), F32),
            vmem((3, heads, HD), F32),
            vmem((n_rep, 3, heads, HD), F32),
            vmem((heads, HD), F32),
            vmem((n_seq, heads, HD), F32),
            vmem((seq_count, q_cols), F32),
            vmem((seq_count, cols), F32),
            vmem((n_head, seq_count, cols), F32),
            vmem((n_ring, 1, 2 * piece + HD), F32),
            vmem((n_ring, 1, 2 * piece + HD), F32),
            vmem((1, piece), F32),
            vmem((n_ring, 1, piece), F32),
            vmem((seq_count, n_rep * piece), F32),
            vmem((seq_count, cols), F32),
            vmem((n_head, seq_count, cols), F32),
            vmem((seq_count, cols), F32),
            dma((8,)),
        ]
        + [dma((count,)) for count in (n_head, n_seq, n_ring, n_rep, n_seq, n_head, n_ring, n_ring, n_head) for _ in range(2)],
        compiler_params=pltpu.CompilerParams(
            collective_id=0, has_side_effects=True, vmem_limit_bytes=60 * 1024 * 1024
        ),
    )(
        lengths,
        pool_row,
        block_table,
        trig_rows(lengths),
        tokens,
        attn_gain[None, :],
        ffn_gain[None, :],
        *weights,
        kv_pool,
    )
    return out, kv


def solution(mesh):
    in_specs = (
        P("groups", ("seq", "rep")),
        P(("seq", "rep")),
        P(("seq", "rep")),
        P(("seq", "rep"), "head"),
        P(("seq", "rep"), "head"),
        P(("seq", "rep"), "head"),
        P("head", ("seq", "rep")),
        P(("seq", "rep"), "head"),
        P(("seq", "rep"), "head"),
        P("head", ("seq", "rep")),
        P(None, ("groups", "seq"), "head", "rep", None),
        P("groups"),
        P("groups"),
        P("groups", None),
    )
    out_specs = (P("groups", ("seq", "rep")), P(None, "groups", ("seq", "rep"), "head"))
    sizes = [mesh.shape[name] for name in ("groups", "seq", "head", "rep")]
    return jax.shard_map(
        functools.partial(shards, *sizes),
        mesh=mesh,
        in_specs=in_specs,
        out_specs=out_specs,
        check_vma=False,
    )
```

```python
import functools
import math

import jax
import jax.numpy as jnp
from jax import lax
from jax.experimental import pallas as pl
from jax.experimental.pallas import tpu as pltpu
from jax.sharding import PartitionSpec as P

HD = 128
EPSILON = 1e-05
ROPE_LOG = math.log(500000.0)
FLOOR_SCORE = -1e30
MESH = pl.DeviceIdType.MESH
F32 = jnp.float32
BF16 = jnp.bfloat16


def round_up(count, unit):
    return -(-count // unit) * unit


def trig_rows(length):
    half_dim = HD // 2
    lane = lax.broadcasted_iota(jnp.int32, (8, HD), 1)
    index = jnp.where(lane < half_dim, lane, lane - half_dim).astype(F32)
    angles = length.astype(F32) * jnp.exp(index * (-2.0 * ROPE_LOG / HD))
    sine_part = jnp.sin(angles)
    return jnp.cos(angles)[0:1], jnp.where(lane < half_dim, -sine_part, sine_part)[0:1]


def high_low(values):
    high = values.astype(BF16).astype(F32)
    return high, values - high


def layer_kernel(
    dims,
    lengths_ref,
    row_ref,
    table_ref,
    tokens_ref,
    gain_ref,
    ffn_gain_ref,
    wq_hbm,
    wk_hbm,
    wv_hbm,
    wo_hbm,
    wg_hbm,
    wu_hbm,
    wd_hbm,
    pool_hbm,
    final,
    arr,
    wq,
    wk,
    wv,
    wo,
    wg,
    wu,
    wd,
    kvx,
    kvs,
    tok,
    xp,
    qkv_part,
    qkv_recv,
    qkv_send_buf,
    split_buf,
    soft_part,
    soft_recv,
    attn_part,
    attn_recv,
    attn_rows,
    proj_part,
    proj_recv,
    mid_part,
    mid_send_buf,
    mid_recv,
    hid_part,
    hid_recv,
    hid_rows,
    down_part,
    down_recv,
    local_sem,
    kvx_send,
    kvx_recv,
    kvz_send,
    kvz_recv,
    kvz_send2,
    kvz_recv2,
    qkv_send,
    qkv_rsem,
    soft_send,
    soft_rsem,
    attn_send,
    attn_rsem,
    proj_send,
    proj_rsem,
    mid_send,
    mid_rsem,
    hid_send,
    hid_rsem,
    down_send,
    down_rsem,
):
    n_seq, n_head, n_rep, width, block = dims
    seq_count = tokens_ref.shape[0]
    group = lax.axis_index("groups")
    s_me = lax.axis_index("seq")
    h_me = lax.axis_index("head")
    r_me = lax.axis_index("rep")
    n_ring = n_seq * n_rep
    me = s_me * n_rep + r_me

    def at_ring(peer):
        return (group, peer // n_rep, h_me, peer % n_rep)

    def at_head(peer):
        return (group, s_me, peer, r_me)

    def at_seq(peer):
        return (group, peer, h_me, r_me)

    def at_rep(peer):
        return (group, s_me, h_me, peer)

    def send_all(source_of, dst, count, mine, place, send, recv):
        copies = []
        for k in range(1, count):
            peer = lax.rem(mine + k, count)
            copy = pltpu.make_async_remote_copy(
                src_ref=source_of(peer),
                dst_ref=dst.at[mine],
                send_sem=send.at[k],
                recv_sem=recv.at[k],
                device_id=place(peer),
                device_id_type=MESH,
            )
            copy.start()
            copies.append(copy)
        return copies

    def arrive(copies):
        for copy in copies:
            copy.wait()

    half_feat = pool_hbm.shape[4] // n_head
    weights = []
    for j, (src, dst) in enumerate(
        ((wq_hbm, wq), (wk_hbm, wk), (wv_hbm, wv), (wo_hbm, wo), (wg_hbm, wg), (wu_hbm, wu), (wd_hbm, wd))
    ):
        copy = pltpu.make_async_copy(src, dst, local_sem.at[j])
        copy.start()
        weights.append(copy)

    def features_for(peer):
        return pool_hbm.at[:, 0, :, :, pl.ds(pl.multiple_of(peer * half_feat, HD), half_feat)]

    own_kv = pltpu.make_async_copy(features_for(h_me), kvx.at[h_me], local_sem.at[7])
    own_kv.start()

    barrier = pltpu.get_barrier_semaphore()
    for k in range(1, n_ring):
        pl.semaphore_signal(
            barrier, inc=1, device_id=at_ring(lax.rem(me + k, n_ring)), device_id_type=MESH
        )
    for k in range(1, n_head):
        pl.semaphore_signal(
            barrier, inc=1, device_id=at_head(lax.rem(h_me + k, n_head)), device_id_type=MESH
        )
    pl.semaphore_wait(barrier, n_ring + n_head - 2)

    kvx_copies = send_all(features_for, kvx, n_head, h_me, at_head, kvx_send, kvx_recv)

    qkv_part[...] = jnp.zeros_like(qkv_part)
    mid_part[...] = jnp.zeros_like(mid_part)
    tok[...] = tokens_ref[...].astype(F32)
    owner_here = jnp.int32(0)
    for p in range(seq_count):
        owner = jnp.int32(0)
        for i in range(seq_count):
            owner = jnp.where(row_ref[i] == p, i, owner)
        owner_here = jnp.where(s_me == p, owner, owner_here)
        xp[p : p + 1, :] = tok[pl.ds(owner, 1), :]
    length_here = lengths_ref[owner_here]

    residual = xp[...]
    square_parts = high_low(jnp.sum(residual * residual, axis=1, keepdims=True))
    trig_cos, trig_sin = trig_rows(length_here)
    heads = wq.shape[1] // HD
    kv_heads = wk.shape[1] // HD

    def projected(values):
        high, low = high_low(values)
        split_buf[0:seq_count, :] = high
        split_buf[seq_count : 2 * seq_count, :] = low
        return split_buf[...].astype(BF16)

    def product(operand, weight):
        both = jnp.dot(operand, weight[...], preferred_element_type=F32)
        return both[0:seq_count] + both[seq_count : 2 * seq_count]

    scaled = projected(residual * gain_ref[...])
    at = 0
    for j, weight in enumerate((wq, wk, wv)):
        weights[j].wait()
        partial = product(scaled, weight)
        for t in range(weight.shape[1] // HD):
            for s in range(seq_count):
                qkv_part[s, at : at + 1, :] = partial[s : s + 1, t * HD : (t + 1) * HD]
            at += 1
    for part in square_parts:
        for s in range(seq_count):
            qkv_part[s, at : at + 1, :] = jnp.broadcast_to(part[s : s + 1], (1, HD))
        at += 1
    qkv_send_buf[...] = qkv_part[...].astype(BF16)
    qkv_recv[me] = qkv_send_buf[s_me]
    qkv_copies = send_all(
        lambda peer: qkv_send_buf.at[peer // n_rep], qkv_recv, n_ring, me, at_ring, qkv_send, qkv_rsem
    )

    own_kv.wait()
    arrive(kvx_copies)
    slots_local = kvx.shape[2]
    half_rows = kvx.shape[3]
    blocks = table_ref.shape[1]
    for c in range(2):
        for b in range(blocks):
            slot = table_ref[owner_here, b]
            holder = slot // slots_local
            local = lax.rem(slot, slots_local)
            first = b * block + r_me * half_rows
            live = lax.broadcasted_iota(jnp.int32, (half_rows, half_feat), 0) + first < length_here
            rows = kvx[holder, c, local].astype(F32)
            kvs[c, b] = jnp.where(live, rows, 0.0).astype(BF16)
        if c == 0:
            key_copies = send_all(
                lambda peer: kvs.at[0, peer], arr.at[0], n_seq, s_me, at_seq, kvz_send, kvz_recv
            )
    kept = pltpu.make_async_copy(kvs.at[:, s_me], arr.at[:, s_me], local_sem.at[8])
    kept.start()

    arrive(qkv_copies)
    summed = jnp.sum(qkv_recv[...].astype(F32), axis=0)
    total = heads + 2 * kv_heads
    scale = lax.rsqrt((summed[total : total + 1] + summed[total + 1 : total + 2]) / width + EPSILON)
    summed = summed * scale
    queries = summed[0:heads]
    keys_new = summed[heads : heads + kv_heads]
    values_new = summed[heads + kv_heads : total].astype(BF16).astype(F32)

    def rotated(values):
        return (values * trig_cos + pltpu.roll(values, HD // 2, 1) * trig_sin).astype(BF16)

    rot_queries = rotated(queries)
    rot_keys = rotated(keys_new).astype(F32)
    factor = 1.0 / math.sqrt(HD)
    per_group = heads // kv_heads
    tokens_here = blocks * half_rows
    spot = lax.broadcasted_iota(jnp.int32, (per_group, tokens_here), 1)
    position = (spot // half_rows) * block + lax.rem(spot, half_rows) + r_me * half_rows
    usable = position < length_here
    for g in range(kv_heads):
        cols = slice(g * HD, (g + 1) * HD)
        mine = slice(g * per_group, (g + 1) * per_group)
        keys = kvs[0, :, :, cols].reshape(tokens_here, HD)
        values = kvs[1, :, :, cols].reshape(tokens_here, HD)
        scores = (
            lax.dot_general(
                rot_queries[mine], keys, (((1,), (1,)), ((), ())), preferred_element_type=F32
            )
            * factor
        )
        scores = jnp.where(usable, scores, FLOOR_SCORE)
        highest = jnp.max(scores, axis=1, keepdims=True)
        shares = jnp.where(usable, jnp.exp(scores - highest), 0.0)
        mass = jnp.sum(shares, axis=1, keepdims=True)
        soft_part[0, mine, :] = jnp.dot(shares.astype(BF16), values, preferred_element_type=F32)
        soft_part[1, mine, :] = jnp.broadcast_to(highest, (per_group, HD))
        soft_part[2, mine, :] = jnp.broadcast_to(mass, (per_group, HD))
    soft_copies = send_all(
        lambda peer: soft_part, soft_recv, n_rep, r_me, at_rep, soft_send, soft_rsem
    )
    soft_recv[r_me] = soft_part[...]
    own_key = jnp.concatenate(
        [jnp.broadcast_to(rot_keys[g : g + 1], (per_group, HD)) for g in range(kv_heads)], axis=0
    )
    own_value = jnp.concatenate(
        [jnp.broadcast_to(values_new[g : g + 1], (per_group, HD)) for g in range(kv_heads)], axis=0
    )
    own_score = jnp.sum(rot_queries.astype(F32) * own_key, axis=1, keepdims=True) * factor
    arrive(soft_copies)
    largest = jnp.broadcast_to(own_score, (heads, HD))
    for r in range(n_rep):
        largest = jnp.maximum(largest, soft_recv[r, 1])
    own_share = jnp.exp(own_score - largest)
    denominator = own_share
    mixed = own_share * own_value
    for r in range(n_rep):
        weight = jnp.exp(soft_recv[r, 1] - largest)
        denominator = denominator + soft_recv[r, 2] * weight
        mixed = mixed + soft_recv[r, 0] * weight
    attn_part[...] = (mixed / denominator).astype(BF16)
    attn_copies = send_all(
        lambda peer: attn_part, attn_recv, n_seq, s_me, at_seq, attn_send, attn_rsem
    )
    attn_recv[s_me] = attn_part[...]
    value_copies = send_all(
        lambda peer: kvs.at[1, peer], arr.at[1], n_seq, s_me, at_seq, kvz_send2, kvz_recv2
    )
    weights[3].wait()
    arrive(attn_copies)
    for s in range(seq_count):
        gathered = attn_recv[s].astype(F32)
        for h in range(heads):
            attn_rows[s : s + 1, h * HD : (h + 1) * HD] = gathered[h : h + 1, :]
    proj_part[...] = jnp.dot(attn_rows[...].astype(BF16), wo[...], preferred_element_type=F32)
    proj_copies = send_all(
        lambda peer: proj_part, proj_recv, n_head, h_me, at_head, proj_send, proj_rsem
    )
    proj_recv[h_me] = proj_part[...]
    for copy in weights[4:6]:
        copy.wait()
    arrive(proj_copies)
    middle = xp[...] + jnp.sum(proj_recv[...], axis=0)
    mid_parts = high_low(jnp.sum(middle * middle, axis=1, keepdims=True))
    mid_scaled = projected(middle * ffn_gain_ref[...])
    tiles = wg.shape[1] // (n_rep * HD)
    up_at = round_up(tiles + 2, 16)
    for weight, start in ((wg, 0), (wu, up_at)):
        partial = product(mid_scaled, weight)
        for s in range(seq_count):
            for r in range(n_rep):
                for t in range(tiles):
                    col = (r * tiles + t) * HD
                    mid_part[s * n_rep + r, start + t : start + t + 1, :] = partial[
                        s : s + 1, col : col + HD
                    ]
    for j, part in enumerate(mid_parts):
        for s in range(seq_count):
            for r in range(n_rep):
                mid_part[s * n_rep + r, tiles + j : tiles + j + 1, :] = jnp.broadcast_to(
                    part[s : s + 1], (1, HD)
                )
    mid_send_buf[...] = mid_part[...].astype(BF16)
    mid_recv[me] = mid_send_buf[me]
    mid_copies = send_all(
        lambda peer: mid_send_buf.at[peer], mid_recv, n_ring, me, at_ring, mid_send, mid_rsem
    )
    arrive(mid_copies)
    sums = jnp.sum(mid_recv[...].astype(F32), axis=0)
    mid_scale = lax.rsqrt((sums[tiles : tiles + 1] + sums[tiles + 1 : tiles + 2]) / width + EPSILON)
    tall = round_up(tiles, 16)
    gate = sums[0:tall] * mid_scale
    up = sums[up_at : up_at + tall] * mid_scale
    hid_part[...] = (gate / (1.0 + jnp.exp(-gate)) * up).astype(BF16)
    hid_copies = send_all(
        lambda peer: hid_part, hid_recv, n_ring, me, at_ring, hid_send, hid_rsem
    )
    hid_recv[me] = hid_part[...]
    weights[6].wait()
    arrive(hid_copies)
    for s in range(seq_count):
        for r in range(n_rep):
            gathered = hid_recv[s * n_rep + r].astype(F32)
            for t in range(tiles):
                col = (r * tiles + t) * HD
                hid_rows[s : s + 1, col : col + HD] = gathered[t : t + 1, :]
    down_part[...] = jnp.dot(hid_rows[...].astype(BF16), wd[...], preferred_element_type=F32)
    down_copies = send_all(
        lambda peer: down_part, down_recv, n_head, h_me, at_head, down_send, down_rsem
    )
    down_recv[h_me] = down_part[...]
    arrive(key_copies)
    arrive(value_copies)
    kept.wait()
    arrive(down_copies)
    final[...] = middle + jnp.sum(down_recv[...], axis=0)


def order_kernel(row_ref, final, arr, out_ref, kv_ref, held, ordered, load_sem, store_sem):
    seq_count = final.shape[0]
    loads, stores = [], []
    for i in range(seq_count):
        copy = pltpu.make_async_copy(arr.at[:, row_ref[i]], held.at[:, i], load_sem.at[i])
        copy.start()
        loads.append(copy)
    for i in range(seq_count):
        ordered[i : i + 1, :] = final[pl.ds(row_ref[i], 1), :]
    out_ref[...] = ordered[...].astype(BF16)
    for i in range(seq_count):
        loads[i].wait()
        copy = pltpu.make_async_copy(held.at[:, i], kv_ref.at[:, i], store_sem.at[i])
        copy.start()
        stores.append(copy)
    for copy in stores:
        copy.wait()


def shards(
    n_groups,
    n_seq,
    n_head,
    n_rep,
    tokens,
    attn_gain,
    ffn_gain,
    w_query,
    w_key,
    w_value,
    w_out,
    w_gate,
    w_up,
    w_down,
    kv_pool,
    lengths,
    pool_row,
    block_table,
):
    seq_count, cols = tokens.shape
    n_ring = n_seq * n_rep
    width = cols * n_ring
    _, _, slots_local, half_rows, feat = kv_pool.shape
    half_feat = feat // n_head
    blocks = block_table.shape[1]
    q_cols, kv_cols = w_query.shape[1], w_key.shape[1]
    heads, kv_heads = q_cols // HD, kv_cols // HD
    qkv = round_up(heads + 2 * kv_heads + 2, 16)
    tiles = w_gate.shape[1] // (n_rep * HD)
    tall = round_up(tiles, 16)
    mid = round_up(tiles + 2, 16) + tall
    vmem = pltpu.VMEM
    dma = pltpu.SemaphoreType.DMA
    hbm = pl.BlockSpec(memory_space=pltpu.HBM)
    in_v = pl.BlockSpec(memory_space=pltpu.VMEM)
    in_s = pl.BlockSpec(memory_space=pltpu.SMEM)
    weights = (w_query, w_key, w_value, w_out, w_gate, w_up, w_down)
    final, arr = pl.pallas_call(
        functools.partial(layer_kernel, (n_seq, n_head, n_rep, width, half_rows * n_rep)),
        out_shape=(
            jax.ShapeDtypeStruct((seq_count, cols), F32),
            jax.ShapeDtypeStruct((2, n_seq, half_rows, half_feat), BF16),
        ),
        in_specs=[in_s] * 3 + [in_v] * 3 + [hbm] * 8,
        out_specs=(in_v, hbm),
        scratch_shapes=[vmem(w.shape, BF16) for w in weights]
        + [
            vmem((n_head, 2, slots_local, half_rows, half_feat), BF16),
            vmem((2, blocks, half_rows, half_feat), BF16),
            vmem((seq_count, cols), F32),
            vmem((seq_count, cols), F32),
            vmem((seq_count, qkv, HD), F32),
            vmem((n_ring, qkv, HD), BF16),
            vmem((seq_count, qkv, HD), BF16),
            vmem((2 * seq_count, cols), F32),
            vmem((3, heads, HD), F32),
            vmem((n_rep, 3, heads, HD), F32),
            vmem((heads, HD), BF16),
            vmem((n_seq, heads, HD), BF16),
            vmem((seq_count, q_cols), F32),
            vmem((seq_count, cols), F32),
            vmem((n_head, seq_count, cols), F32),
            vmem((n_ring, mid, HD), F32),
            vmem((n_ring, mid, HD), BF16),
            vmem((n_ring, mid, HD), BF16),
            vmem((tall, HD), BF16),
            vmem((n_ring, tall, HD), BF16),
            vmem((seq_count, w_gate.shape[1]), F32),
            vmem((seq_count, cols), F32),
            vmem((n_head, seq_count, cols), F32),
            dma((9,)),
        ]
        + [dma((count,)) for count in (n_head, n_seq, n_seq, n_ring, n_rep, n_seq, n_head, n_ring, n_ring, n_head) for _ in range(2)],
        compiler_params=pltpu.CompilerParams(
            collective_id=0, has_side_effects=True, vmem_limit_bytes=60 * 1024 * 1024
        ),
    )(
        lengths,
        pool_row,
        block_table,
        tokens,
        attn_gain[None, :],
        ffn_gain[None, :],
        *weights,
        kv_pool,
    )
    return pl.pallas_call(
        order_kernel,
        out_shape=(
            jax.ShapeDtypeStruct((seq_count, cols), BF16),
            jax.ShapeDtypeStruct((2, seq_count, half_rows, half_feat), BF16),
        ),
        in_specs=[in_s, in_v, hbm],
        out_specs=(in_v, hbm),
        scratch_shapes=[
            vmem((2, seq_count, half_rows, half_feat), BF16),
            vmem((seq_count, cols), F32),
            dma((seq_count,)),
            dma((seq_count,)),
        ],
    )(pool_row, final, arr)


def solution(mesh):
    in_specs = (
        P("groups", ("seq", "rep")),
        P(("seq", "rep")),
        P(("seq", "rep")),
        P(("seq", "rep"), "head"),
        P(("seq", "rep"), "head"),
        P(("seq", "rep"), "head"),
        P("head", ("seq", "rep")),
        P(("seq", "rep"), "head"),
        P(("seq", "rep"), "head"),
        P("head", ("seq", "rep")),
        P(None, ("groups", "seq"), "head", "rep", None),
        P("groups"),
        P("groups"),
        P("groups", None),
    )
    out_specs = (P("groups", ("seq", "rep")), P(None, "groups", ("seq", "rep"), "head"))
    sizes = [mesh.shape[name] for name in ("groups", "seq", "head", "rep")]
    return jax.shard_map(
        functools.partial(shards, *sizes),
        mesh=mesh,
        in_specs=in_specs,
        out_specs=out_specs,
        check_vma=False,
    )
```

```python
import functools
import math

import jax
import jax.numpy as jnp
from jax import lax
from jax.experimental import pallas as pl
from jax.experimental.pallas import tpu as pltpu
from jax.sharding import PartitionSpec as P

HD = 128
EPSILON = 1e-05
ROPE_LOG = math.log(500000.0)
FLOOR_SCORE = -1e30
MESH = pl.DeviceIdType.MESH
F32 = jnp.float32
BF16 = jnp.bfloat16


def round_up(count, unit):
    return -(-count // unit) * unit


def trig_rows(length):
    half_dim = HD // 2
    lane = lax.broadcasted_iota(jnp.int32, (8, HD), 1)
    index = jnp.where(lane < half_dim, lane, lane - half_dim).astype(F32)
    angles = length.astype(F32) * jnp.exp(index * (-2.0 * ROPE_LOG / HD))
    sine_part = jnp.sin(angles)
    return jnp.cos(angles)[0:1], jnp.where(lane < half_dim, -sine_part, sine_part)[0:1]


def high_low(values):
    high = values.astype(BF16).astype(F32)
    return high, values - high


def layer_kernel(
    dims,
    lengths_ref,
    row_ref,
    table_ref,
    tokens_ref,
    gain_ref,
    ffn_gain_ref,
    wq_hbm,
    wk_hbm,
    wv_hbm,
    wo_hbm,
    wg_hbm,
    wu_hbm,
    wd_hbm,
    pool_hbm,
    final,
    arr,
    wq,
    wk,
    wv,
    wo,
    wg,
    wu,
    wd,
    kvx,
    kvs,
    tok,
    xp,
    qkv_part,
    qkv_recv,
    qkv_send_buf,
    split_buf,
    soft_part,
    soft_recv,
    attn_part,
    attn_recv,
    attn_rows,
    proj_part,
    proj_recv,
    mid_part,
    mid_send_buf,
    mid_recv,
    hid_part,
    hid_recv,
    hid_rows,
    down_part,
    down_recv,
    local_sem,
    kvx_send,
    kvx_recv,
    kvz_send,
    kvz_recv,
    kvz_send2,
    kvz_recv2,
    kvz_send3,
    kvz_recv3,
    qkv_send,
    qkv_rsem,
    soft_send,
    soft_rsem,
    attn_send,
    attn_rsem,
    proj_send,
    proj_rsem,
    mid_send,
    mid_rsem,
    hid_send,
    hid_rsem,
    down_send,
    down_rsem,
):
    n_seq, n_head, n_rep, width, block = dims
    seq_count = tokens_ref.shape[0]
    group = lax.axis_index("groups")
    s_me = lax.axis_index("seq")
    h_me = lax.axis_index("head")
    r_me = lax.axis_index("rep")
    n_ring = n_seq * n_rep
    me = s_me * n_rep + r_me

    def at_ring(peer):
        return (group, peer // n_rep, h_me, peer % n_rep)

    def at_head(peer):
        return (group, s_me, peer, r_me)

    def at_seq(peer):
        return (group, peer, h_me, r_me)

    def at_rep(peer):
        return (group, s_me, h_me, peer)

    def send_all(source_of, dst, count, mine, place, send, recv):
        copies = []
        for k in range(1, count):
            peer = lax.rem(mine + k, count)
            copy = pltpu.make_async_remote_copy(
                src_ref=source_of(peer),
                dst_ref=dst.at[mine],
                send_sem=send.at[k],
                recv_sem=recv.at[k],
                device_id=place(peer),
                device_id_type=MESH,
            )
            copy.start()
            copies.append(copy)
        return copies

    def arrive(copies):
        for copy in copies:
            copy.wait()

    half_feat = pool_hbm.shape[4] // n_head
    weights = []
    for j, (src, dst) in enumerate(
        ((wq_hbm, wq), (wk_hbm, wk), (wv_hbm, wv), (wo_hbm, wo), (wg_hbm, wg), (wu_hbm, wu), (wd_hbm, wd))
    ):
        copy = pltpu.make_async_copy(src, dst, local_sem.at[j])
        if j < 3:
            copy.start()
        weights.append(copy)

    def features_for(peer):
        return pool_hbm.at[:, 0, :, :, pl.ds(pl.multiple_of(peer * half_feat, HD), half_feat)]

    own_kv = pltpu.make_async_copy(features_for(h_me), kvx.at[h_me], local_sem.at[7])
    own_kv.start()

    barrier = pltpu.get_barrier_semaphore()
    for k in range(1, n_ring):
        pl.semaphore_signal(
            barrier, inc=1, device_id=at_ring(lax.rem(me + k, n_ring)), device_id_type=MESH
        )
    for k in range(1, n_head):
        pl.semaphore_signal(
            barrier, inc=1, device_id=at_head(lax.rem(h_me + k, n_head)), device_id_type=MESH
        )
    pl.semaphore_wait(barrier, n_ring + n_head - 2)

    kvx_copies = send_all(features_for, kvx, n_head, h_me, at_head, kvx_send, kvx_recv)

    qkv_part[...] = jnp.zeros_like(qkv_part)
    mid_part[...] = jnp.zeros_like(mid_part)
    tok[...] = tokens_ref[...].astype(F32)
    owner_here = jnp.int32(0)
    for p in range(seq_count):
        owner = jnp.int32(0)
        for i in range(seq_count):
            owner = jnp.where(row_ref[i] == p, i, owner)
        owner_here = jnp.where(s_me == p, owner, owner_here)
        xp[p : p + 1, :] = tok[pl.ds(owner, 1), :]
    length_here = lengths_ref[owner_here]

    residual = xp[...]
    square_parts = high_low(jnp.sum(residual * residual, axis=1, keepdims=True))
    trig_cos, trig_sin = trig_rows(length_here)
    heads = wq.shape[1] // HD
    kv_heads = wk.shape[1] // HD

    def projected(values):
        high, low = high_low(values)
        split_buf[0:seq_count, :] = high
        split_buf[seq_count : 2 * seq_count, :] = low
        return split_buf[...].astype(BF16)

    def product(operand, weight):
        both = jnp.dot(operand, weight[...], preferred_element_type=F32)
        return both[0:seq_count] + both[seq_count : 2 * seq_count]

    scaled = projected(residual * gain_ref[...])
    at = 0
    for j, weight in enumerate((wq, wk, wv)):
        weights[j].wait()
        partial = product(scaled, weight)
        for t in range(weight.shape[1] // HD):
            for s in range(seq_count):
                qkv_part[s, at : at + 1, :] = partial[s : s + 1, t * HD : (t + 1) * HD]
            at += 1
    for part in square_parts:
        for s in range(seq_count):
            qkv_part[s, at : at + 1, :] = jnp.broadcast_to(part[s : s + 1], (1, HD))
        at += 1
    for copy in weights[3:]:
        copy.start()
    qkv_send_buf[...] = qkv_part[...].astype(BF16)
    qkv_recv[me] = qkv_send_buf[s_me]
    qkv_copies = send_all(
        lambda peer: qkv_send_buf.at[peer // n_rep], qkv_recv, n_ring, me, at_ring, qkv_send, qkv_rsem
    )

    own_kv.wait()
    arrive(kvx_copies)
    slots_local = kvx.shape[2]
    half_rows = kvx.shape[3]
    blocks = table_ref.shape[1]
    for c in range(2):
        for b in range(blocks):
            slot = table_ref[owner_here, b]
            holder = slot // slots_local
            local = lax.rem(slot, slots_local)
            first = b * block + r_me * half_rows
            live = lax.broadcasted_iota(jnp.int32, (half_rows, half_feat), 0) + first < length_here
            rows = kvx[holder, c, local].astype(F32)
            kvs[c, b] = jnp.where(live, rows, 0.0).astype(BF16)
    kept = pltpu.make_async_copy(kvs.at[:, s_me], arr.at[:, s_me], local_sem.at[8])
    kept.start()

    arrive(qkv_copies)
    summed = jnp.sum(qkv_recv[...].astype(F32), axis=0)
    total = heads + 2 * kv_heads
    scale = lax.rsqrt((summed[total : total + 1] + summed[total + 1 : total + 2]) / width + EPSILON)
    summed = summed * scale
    queries = summed[0:heads]
    keys_new = summed[heads : heads + kv_heads]
    values_new = summed[heads + kv_heads : total].astype(BF16).astype(F32)

    def rotated(values):
        return (values * trig_cos + pltpu.roll(values, HD // 2, 1) * trig_sin).astype(BF16)

    rot_queries = rotated(queries)
    rot_keys = rotated(keys_new).astype(F32)
    factor = 1.0 / math.sqrt(HD)
    per_group = heads // kv_heads
    tokens_here = blocks * half_rows
    spot = lax.broadcasted_iota(jnp.int32, (per_group, tokens_here), 1)
    position = (spot // half_rows) * block + lax.rem(spot, half_rows) + r_me * half_rows
    usable = position < length_here
    for g in range(kv_heads):
        cols = slice(g * HD, (g + 1) * HD)
        mine = slice(g * per_group, (g + 1) * per_group)
        keys = kvs[0, :, :, cols].reshape(tokens_here, HD)
        values = kvs[1, :, :, cols].reshape(tokens_here, HD)
        scores = (
            lax.dot_general(
                rot_queries[mine], keys, (((1,), (1,)), ((), ())), preferred_element_type=F32
            )
            * factor
        )
        scores = jnp.where(usable, scores, FLOOR_SCORE)
        highest = jnp.max(scores, axis=1, keepdims=True)
        shares = jnp.where(usable, jnp.exp(scores - highest), 0.0)
        mass = jnp.sum(shares, axis=1, keepdims=True)
        soft_part[0, mine, :] = jnp.dot(shares.astype(BF16), values, preferred_element_type=F32)
        soft_part[1, mine, :] = jnp.broadcast_to(highest, (per_group, HD))
        soft_part[2, mine, :] = jnp.broadcast_to(mass, (per_group, HD))
    soft_copies = send_all(
        lambda peer: soft_part, soft_recv, n_rep, r_me, at_rep, soft_send, soft_rsem
    )
    soft_recv[r_me] = soft_part[...]
    own_key = jnp.concatenate(
        [jnp.broadcast_to(rot_keys[g : g + 1], (per_group, HD)) for g in range(kv_heads)], axis=0
    )
    own_value = jnp.concatenate(
        [jnp.broadcast_to(values_new[g : g + 1], (per_group, HD)) for g in range(kv_heads)], axis=0
    )
    own_score = jnp.sum(rot_queries.astype(F32) * own_key, axis=1, keepdims=True) * factor
    arrive(soft_copies)
    largest = jnp.broadcast_to(own_score, (heads, HD))
    for r in range(n_rep):
        largest = jnp.maximum(largest, soft_recv[r, 1])
    own_share = jnp.exp(own_score - largest)
    denominator = own_share
    mixed = own_share * own_value
    for r in range(n_rep):
        weight = jnp.exp(soft_recv[r, 1] - largest)
        denominator = denominator + soft_recv[r, 2] * weight
        mixed = mixed + soft_recv[r, 0] * weight
    attn_part[...] = (mixed / denominator).astype(BF16)
    attn_copies = send_all(
        lambda peer: attn_part, attn_recv, n_seq, s_me, at_seq, attn_send, attn_rsem
    )
    attn_recv[s_me] = attn_part[...]
    part_rows = half_rows // 2
    early_copies = send_all(
        lambda peer: kvs.at[0, peer], arr.at[0], n_seq, s_me, at_seq, kvz_send, kvz_recv
    )
    early_copies += send_all(
        lambda peer: kvs.at[1, peer, pl.ds(0, part_rows)],
        arr.at[1, :, pl.ds(0, part_rows)],
        n_seq,
        s_me,
        at_seq,
        kvz_send2,
        kvz_recv2,
    )
    weights[3].wait()
    arrive(attn_copies)
    for s in range(seq_count):
        gathered = attn_recv[s].astype(F32)
        for h in range(heads):
            attn_rows[s : s + 1, h * HD : (h + 1) * HD] = gathered[h : h + 1, :]
    proj_part[...] = jnp.dot(attn_rows[...].astype(BF16), wo[...], preferred_element_type=F32)
    proj_copies = send_all(
        lambda peer: proj_part, proj_recv, n_head, h_me, at_head, proj_send, proj_rsem
    )
    proj_recv[h_me] = proj_part[...]
    for copy in weights[4:6]:
        copy.wait()
    arrive(proj_copies)
    middle = xp[...] + jnp.sum(proj_recv[...], axis=0)
    mid_parts = high_low(jnp.sum(middle * middle, axis=1, keepdims=True))
    mid_scaled = projected(middle * ffn_gain_ref[...])
    tiles = wg.shape[1] // (n_rep * HD)
    up_at = round_up(tiles + 2, 16)
    for weight, start in ((wg, 0), (wu, up_at)):
        partial = product(mid_scaled, weight)
        for s in range(seq_count):
            for r in range(n_rep):
                for t in range(tiles):
                    col = (r * tiles + t) * HD
                    mid_part[s * n_rep + r, start + t : start + t + 1, :] = partial[
                        s : s + 1, col : col + HD
                    ]
    for j, part in enumerate(mid_parts):
        for s in range(seq_count):
            for r in range(n_rep):
                mid_part[s * n_rep + r, tiles + j : tiles + j + 1, :] = jnp.broadcast_to(
                    part[s : s + 1], (1, HD)
                )
    mid_send_buf[...] = mid_part[...].astype(BF16)
    mid_recv[me] = mid_send_buf[me]
    mid_copies = send_all(
        lambda peer: mid_send_buf.at[peer], mid_recv, n_ring, me, at_ring, mid_send, mid_rsem
    )
    late_copies = send_all(
        lambda peer: kvs.at[1, peer, pl.ds(part_rows, part_rows)],
        arr.at[1, :, pl.ds(part_rows, part_rows)],
        n_seq,
        s_me,
        at_seq,
        kvz_send3,
        kvz_recv3,
    )
    arrive(mid_copies)
    sums = jnp.sum(mid_recv[...].astype(F32), axis=0)
    mid_scale = lax.rsqrt((sums[tiles : tiles + 1] + sums[tiles + 1 : tiles + 2]) / width + EPSILON)
    tall = round_up(tiles, 16)
    gate = sums[0:tall] * mid_scale
    up = sums[up_at : up_at + tall] * mid_scale
    hid_part[...] = (gate / (1.0 + jnp.exp(-gate)) * up).astype(BF16)
    hid_copies = send_all(
        lambda peer: hid_part, hid_recv, n_ring, me, at_ring, hid_send, hid_rsem
    )
    hid_recv[me] = hid_part[...]
    weights[6].wait()
    arrive(hid_copies)
    for s in range(seq_count):
        for r in range(n_rep):
            gathered = hid_recv[s * n_rep + r].astype(F32)
            for t in range(tiles):
                col = (r * tiles + t) * HD
                hid_rows[s : s + 1, col : col + HD] = gathered[t : t + 1, :]
    down_part[...] = jnp.dot(hid_rows[...].astype(BF16), wd[...], preferred_element_type=F32)
    down_copies = send_all(
        lambda peer: down_part, down_recv, n_head, h_me, at_head, down_send, down_rsem
    )
    down_recv[h_me] = down_part[...]
    arrive(early_copies)
    arrive(late_copies)
    kept.wait()
    arrive(down_copies)
    final[...] = middle + jnp.sum(down_recv[...], axis=0)


def order_kernel(row_ref, final, arr, out_ref, kv_ref, ordered, store_sem):
    seq_count = final.shape[0]
    stores = []
    for i in range(seq_count):
        copy = pltpu.make_async_copy(arr.at[:, row_ref[i]], kv_ref.at[:, i], store_sem.at[i])
        copy.start()
        stores.append(copy)
    for i in range(seq_count):
        ordered[i : i + 1, :] = final[pl.ds(row_ref[i], 1), :]
    out_ref[...] = ordered[...].astype(BF16)
    for copy in stores:
        copy.wait()


def shards(
    n_groups,
    n_seq,
    n_head,
    n_rep,
    tokens,
    attn_gain,
    ffn_gain,
    w_query,
    w_key,
    w_value,
    w_out,
    w_gate,
    w_up,
    w_down,
    kv_pool,
    lengths,
    pool_row,
    block_table,
):
    seq_count, cols = tokens.shape
    n_ring = n_seq * n_rep
    width = cols * n_ring
    _, _, slots_local, half_rows, feat = kv_pool.shape
    half_feat = feat // n_head
    blocks = block_table.shape[1]
    q_cols, kv_cols = w_query.shape[1], w_key.shape[1]
    heads, kv_heads = q_cols // HD, kv_cols // HD
    qkv = round_up(heads + 2 * kv_heads + 2, 16)
    tiles = w_gate.shape[1] // (n_rep * HD)
    tall = round_up(tiles, 16)
    mid = round_up(tiles + 2, 16) + tall
    vmem = pltpu.VMEM
    dma = pltpu.SemaphoreType.DMA
    hbm = pl.BlockSpec(memory_space=pltpu.HBM)
    in_v = pl.BlockSpec(memory_space=pltpu.VMEM)
    in_s = pl.BlockSpec(memory_space=pltpu.SMEM)
    weights = (w_query, w_key, w_value, w_out, w_gate, w_up, w_down)
    final, arr = pl.pallas_call(
        functools.partial(layer_kernel, (n_seq, n_head, n_rep, width, half_rows * n_rep)),
        out_shape=(
            jax.ShapeDtypeStruct((seq_count, cols), F32),
            jax.ShapeDtypeStruct((2, n_seq, half_rows, half_feat), BF16),
        ),
        in_specs=[in_s] * 3 + [in_v] * 3 + [hbm] * 8,
        out_specs=(in_v, hbm),
        scratch_shapes=[vmem(w.shape, BF16) for w in weights]
        + [
            vmem((n_head, 2, slots_local, half_rows, half_feat), BF16),
            vmem((2, blocks, half_rows, half_feat), BF16),
            vmem((seq_count, cols), F32),
            vmem((seq_count, cols), F32),
            vmem((seq_count, qkv, HD), F32),
            vmem((n_ring, qkv, HD), BF16),
            vmem((seq_count, qkv, HD), BF16),
            vmem((2 * seq_count, cols), F32),
            vmem((3, heads, HD), F32),
            vmem((n_rep, 3, heads, HD), F32),
            vmem((heads, HD), BF16),
            vmem((n_seq, heads, HD), BF16),
            vmem((seq_count, q_cols), F32),
            vmem((seq_count, cols), F32),
            vmem((n_head, seq_count, cols), F32),
            vmem((n_ring, mid, HD), F32),
            vmem((n_ring, mid, HD), BF16),
            vmem((n_ring, mid, HD), BF16),
            vmem((tall, HD), BF16),
            vmem((n_ring, tall, HD), BF16),
            vmem((seq_count, w_gate.shape[1]), F32),
            vmem((seq_count, cols), F32),
            vmem((n_head, seq_count, cols), F32),
            dma((9,)),
        ]
        + [dma((count,)) for count in (n_head, n_seq, n_seq, n_seq, n_ring, n_rep, n_seq, n_head, n_ring, n_ring, n_head) for _ in range(2)],
        compiler_params=pltpu.CompilerParams(
            collective_id=0, has_side_effects=True, vmem_limit_bytes=60 * 1024 * 1024
        ),
    )(
        lengths,
        pool_row,
        block_table,
        tokens,
        attn_gain[None, :],
        ffn_gain[None, :],
        *weights,
        kv_pool,
    )
    return pl.pallas_call(
        order_kernel,
        out_shape=(
            jax.ShapeDtypeStruct((seq_count, cols), BF16),
            jax.ShapeDtypeStruct((2, seq_count, half_rows, half_feat), BF16),
        ),
        in_specs=[in_s, in_v, in_v],
        out_specs=(in_v, hbm),
        scratch_shapes=[
            vmem((seq_count, cols), F32),
            dma((seq_count,)),
        ],
    )(pool_row, final, arr)


def solution(mesh):
    in_specs = (
        P("groups", ("seq", "rep")),
        P(("seq", "rep")),
        P(("seq", "rep")),
        P(("seq", "rep"), "head"),
        P(("seq", "rep"), "head"),
        P(("seq", "rep"), "head"),
        P("head", ("seq", "rep")),
        P(("seq", "rep"), "head"),
        P(("seq", "rep"), "head"),
        P("head", ("seq", "rep")),
        P(None, ("groups", "seq"), "head", "rep", None),
        P("groups"),
        P("groups"),
        P("groups", None),
    )
    out_specs = (P("groups", ("seq", "rep")), P(None, "groups", ("seq", "rep"), "head"))
    sizes = [mesh.shape[name] for name in ("groups", "seq", "head", "rep")]
    return jax.shard_map(
        functools.partial(shards, *sizes),
        mesh=mesh,
        in_specs=in_specs,
        out_specs=out_specs,
        check_vma=False,
    )
```
